32 devices in a mesh: dp: 1 (over z), tp: 32 (over x, y, core).
Axes of the slice: x: 4, y: 4, z: 1, core: 2. Of those that a mesh axis runs over, the one named last changes fastest.
The devices are a block of a 4x4x8 slice.
Arguments:
- x: bfloat16 [2048, 4096], P('dp')
- dy: bfloat16 [2048, 4096], P('dp')
- gate: bfloat16 [2048, 12288], P('dp', 'tp')
- up: bfloat16 [2048, 12288], P('dp', 'tp')
- w_gate: bfloat16 [4096, 12288], P(None, 'tp')
- w_up: bfloat16 [4096, 12288], P(None, 'tp')
- w_down: bfloat16 [12288, 4096], P('tp')
Outputs:
- output 1: bfloat16 [2048, 4096], P('dp')
- output 2: bfloat16 [4096, 12288], P('dp', 'tp')
- output 3: bfloat16 [4096, 12288], P('dp', 'tp')
- output 4: bfloat16 [12288, 4096], P(('dp', 'tp'))
All inputs are finite; a program needn't handle non-finite values.
Results may differ from the reference program's by a relative error of at most 0.012.
Values are sent between devices in bfloat16 or wider.
A program may use at most 768 MiB of HBM per device.

```python
import jax
import jax.numpy as jnp

ROWS = 2048
D = 4096
FF = 12288


def act(gate, up):
    return jax.nn.silu(gate) * up


def setup_inputs(seed: int = 0, part: int = 0) -> dict:
    kx, ky, ka, kb, kg, ku, kd = jax.random.split(jax.random.key(seed), 7)
    kx, ky, ka, kb = (jax.random.fold_in(k, part) for k in (kx, ky, ka, kb))
    drawn = {
        "x": jax.random.normal(kx, (ROWS, D), jnp.float32),
        "dy": jax.random.normal(ky, (ROWS, D), jnp.float32),
        "gate": jax.random.normal(ka, (ROWS, FF), jnp.float32),
        "up": jax.random.normal(kb, (ROWS, FF), jnp.float32),
        "w_gate": jax.random.normal(kg, (D, FF), jnp.float32) * D**-0.5,
        "w_up": jax.random.normal(ku, (D, FF), jnp.float32) * D**-0.5,
        "w_down": jax.random.normal(kd, (FF, D), jnp.float32) * FF**-0.5,
    }
    return {k: v.astype(jnp.bfloat16) for k, v in drawn.items()}


def reference(x, dy, gate, up, w_gate, w_up, w_down):
    hidden, back = jax.vjp(act, gate.astype(jnp.float32), up.astype(jnp.float32))
    d_hidden = jnp.dot(dy, w_down.T, preferred_element_type=jnp.float32)
    d_gate, d_up = (g.astype(jnp.bfloat16) for g in back(d_hidden))
    dx = jnp.dot(d_gate, w_gate.T, preferred_element_type=jnp.float32) + jnp.dot(d_up, w_up.T, preferred_element_type=jnp.float32)
    dw_gate = jnp.dot(x.T, d_gate, preferred_element_type=jnp.float32)
    dw_up = jnp.dot(x.T, d_up, preferred_element_type=jnp.float32)
    dw_down = jnp.dot(hidden.astype(jnp.bfloat16).T, dy, preferred_element_type=jnp.float32)
    return tuple(g.astype(jnp.bfloat16) for g in (dx, dw_gate, dw_up, dw_down))
```

```python
import functools
import math

import jax
import jax.numpy as jnp
from jax import lax
from jax.experimental import pallas as pl
from jax.experimental.pallas import tpu as pltpu
from jax.sharding import PartitionSpec as P

F32, BF16 = jnp.float32, jnp.bfloat16
STEPS = 16
MIB = 1 << 20


def contract(a, b, ca, cb):
    return lax.dot_general(a, b, (((ca,), (cb,)), ((), ())), preferred_element_type=F32)


def kernel(
    side,
    x_hbm, dy_hbm, gate_hbm, up_hbm, wg_hbm, wu_hbm, wd_hbm,
    dx, dwg, dwu, dwd,
    wd_v, wc_v, gate_v, up_v, row_v, dc_v, ht_v, r1, r2, own, xcol_v, dycol_v,
    w_sem, row_sem, col_sem,
    free, pair_s, pair_r, one_s, one_r, two_s, two_r, ag2_s, ag2_r, ag1_s, ag1_r, agp_s, agp_r,
):
    rows, width = dx.shape
    f = wd_v.shape[0]
    half, hw = rows // 2, width // 2
    gr = half // side
    ur = gr // side
    cb = width // STEPS

    me = lax.axis_index("tp")
    c = lax.rem(me, 2)
    chip = lax.div(me, 2)
    cx, cy = lax.div(chip, side), lax.rem(chip, side)
    p = cx * (1 - c) + cy * c
    q = cy * (1 - c) + cx * c

    def wrap(v):
        return lax.rem(v + side, side)

    def device(pp, qq, cc):
        return {"tp": ((pp * (1 - cc) + qq * cc) * side + (qq * (1 - cc) + pp * cc)) * 2 + cc}

    partner = {"tp": chip * 2 + (1 - c)}
    p_dev = (device(wrap(p + 1), q, c), device(wrap(p - 1), q, c))
    q_dev = (device(p, wrap(q + 1), c), device(p, wrap(q - 1), c))
    offs = (2, 1, -1, 0)
    pg = [wrap(p + o) for o in offs]
    qg = [wrap(q + o) for o in offs]

    def row_of(cc, g, u):
        return pl.multiple_of(cc * half + g * gr + u * ur, ur)

    def remote(src, dst, s, r, dev):
        return pltpu.make_async_remote_copy(
            src_ref=src, dst_ref=dst, send_sem=s, recv_sem=r, device_id=dev, device_id_type=pl.DeviceIdType.MESH
        )

    sent = []

    def send(src, dst, s, r, dev):
        d = remote(src, dst, s, r, dev)
        d.start()
        sent.append(d)

    def arrived(ref, r):
        remote(ref, ref, r, r, partner).wait_recv()

    def lanes(h):
        return pl.ds(h * hw, hw)

    def release(k, devices):
        for d in sent:
            d.wait_send()
        sent.clear()
        for dev in devices:
            pl.semaphore_signal(free.at[k], inc=1, device_id=dev, device_id_type=pl.DeviceIdType.MESH)

    w_copies = [
        pltpu.make_async_copy(wd_hbm, wd_v, w_sem.at[0]),
        pltpu.make_async_copy(wg_hbm, wc_v.at[:, pl.ds(0, f)], w_sem.at[1]),
        pltpu.make_async_copy(wu_hbm, wc_v.at[:, pl.ds(f, f)], w_sem.at[2]),
    ]
    order = [(1 - c, qg[0]), (c, pg[0]), (1 - c, qg[1]), (1 - c, qg[2]), (c, pg[1]), (c, pg[2]), (1 - c, qg[3]), (c, pg[3])]

    def row_copies(i):
        at = pl.ds(row_of(*order[i], 0), gr)
        slot = i % 2
        return [
            pltpu.make_async_copy(dy_hbm.at[at, :], row_v.at[slot], row_sem.at[slot, 0]),
            pltpu.make_async_copy(gate_hbm.at[at, :], gate_v.at[slot], row_sem.at[slot, 1]),
            pltpu.make_async_copy(up_hbm.at[at, :], up_v.at[slot], row_sem.at[slot, 2]),
        ]

    def col_copies(i, slot):
        at = pl.ds(pl.multiple_of(i * cb, cb), cb)
        return [
            pltpu.make_async_copy(x_hbm.at[:, at], xcol_v.at[slot], col_sem.at[slot, 0]),
            pltpu.make_async_copy(dy_hbm.at[:, at], dycol_v.at[slot], col_sem.at[slot, 1]),
        ]

    w_copies[0].start()
    for d in row_copies(0):
        d.start()
    for d in w_copies[1:]:
        d.start()

    barrier = pltpu.get_barrier_semaphore()
    for dev in (partner, *p_dev, *q_dev):
        pl.semaphore_signal(barrier, inc=1, device_id=dev, device_id_type=pl.DeviceIdType.MESH)
    pl.semaphore_wait(barrier, 5)

    w_copies[0].wait()

    def hidden(i):
        slot = i % 2
        if i + 1 < len(order):
            for d in row_copies(i + 1):
                d.start()
        for d in row_copies(i):
            d.wait()
        dh = contract(row_v[slot], wd_v[...], 1, 1)
        g, u = gate_v[slot].astype(F32), up_v[slot].astype(F32)
        s = jax.nn.sigmoid(g)
        silu = g * s
        at = pl.ds(row_of(*order[i], 0), gr)
        dc_v[at, pl.ds(0, f)] = (dh * u * (s + silu * (1.0 - s))).astype(BF16)
        dc_v[at, pl.ds(f, f)] = (dh * silu).astype(BF16)
        ht_v[:, pl.ds(pl.multiple_of(row_of(*order[i], 0), gr), gr)] = (silu * u).astype(BF16).T

    tw = hw // 2

    def term(i, h, finish):
        at = pl.ds(row_of(*order[i], 0), gr)

        @pl.loop(0, hw // tw)
        def _(j):
            col = pl.ds(pl.multiple_of(h * hw + j * tw, tw), tw)
            finish(at, col, pl.ds(pl.multiple_of(j * tw, tw), tw), contract(dc_v[at, :], wc_v[col, :], 1, 1))

    def put(at, col, _, t):
        dx[at, col] = t.astype(BF16)

    def add(at, col, _, t):
        dx[at, col] = (t + dx[at, col].astype(F32)).astype(BF16)

    def add_from(ring):
        def finish(at, col, local, t):
            dx[at, col] = (t + dx[at, col].astype(F32) + ring[:, local].astype(F32)).astype(BF16)

        return finish

    def keep(at, col, _, t):
        own[:, col] = t + dx[at, col].astype(F32)

    def to_partner(i, k):
        for h in range(2):
            term(i, h, put)
            part = dx.at[pl.ds(row_of(*order[i], 0), gr), lanes(h)]
            send(part, part, pair_s.at[k, h], pair_r.at[k, h], partner)

    def from_partner(i, k, h):
        arrived(dx.at[pl.ds(row_of(*order[i], 0), gr), lanes(h)], pair_r.at[k, h])

    def dw_block(i):
        slot = lax.rem(i, 2)

        @pl.when(i + 1 < STEPS)
        def _():
            for d in col_copies(i + 1, 1 - slot):
                d.start()

        for d in col_copies(i, slot):
            d.wait()
        at = pl.ds(pl.multiple_of(i * cb, cb), cb)
        both = contract(xcol_v[slot], dc_v[...], 0, 0).astype(BF16)
        dwg[at, :] = both[:, :f]
        dwu[at, :] = both[:, f:]
        dwd[:, at] = jnp.dot(ht_v[...], dycol_v[slot], preferred_element_type=F32).astype(BF16)

    done = [0]

    def dw(n):
        lo = done[0]
        done[0] = min(STEPS, lo + n)
        pl.loop(lo, done[0])(dw_block)

    hidden(0)
    for d in w_copies[1:]:
        d.wait()
    to_partner(0, 0)
    hidden(1)
    at = pl.ds(row_of(c, pg[0], 0), gr)
    for h, way in ((1, 0), (0, 1)):
        from_partner(1, 0, h)
        term(1, h, add)
        send(dx.at[at, lanes(h)], r1.at[way, 0], one_s.at[way, 0], one_r.at[way, 0], p_dev[way])
    hidden(2)
    to_partner(2, 1)
    hidden(3)
    to_partner(3, 2)
    hidden(4)
    hidden(5)
    for i, k, h, way in ((4, 1, 0, 0), (5, 2, 1, 1)):
        from_partner(i, k, h)
        term(i, h, add)
        at = pl.ds(row_of(*order[i], 0), gr)
        send(dx.at[at, lanes(h)], r1.at[way, 1], one_s.at[way, 1], one_r.at[way, 1], p_dev[way])
    for d in col_copies(0, 0):
        d.start()
    for i, k, h, way in ((4, 1, 1, 0), (5, 2, 0, 1)):
        from_partner(i, k, h)
        arrived(r1.at[way, 0], one_r.at[way, 0])
        term(i, h, add_from(r1.at[way, 0]))
        for s in range(side):
            at = pl.ds(row_of(c, pg[k], qg[s]), ur)
            to = r1.at[way, 2, pl.ds(pl.multiple_of(qg[s] * ur, ur), ur)]
            send(dx.at[at, lanes(h)], to, one_s.at[way, 2 + s], one_r.at[way, 2 + s], p_dev[way])
    hidden(6)
    to_partner(6, 3)
    hidden(7)
    for h in range(2):
        from_partner(7, 3, h)
        term(7, h, keep)
    dw(2)
    for h in range(2):
        arrived(r1.at[h, 1], one_r.at[h, 1])
        own[:, lanes(h)] += r1[h, 1].astype(F32)
    dw(1)

    def unit(s):
        return pl.ds(pl.multiple_of(qg[s] * ur, ur), ur)

    def unit_dx(s):
        return pl.ds(row_of(c, p, qg[s]), ur)

    def close_one(s):
        for h, way in ((1, 0), (0, 1)):
            arrived(r1.at[way, 2, unit(s)], one_r.at[way, 2 + s])
            own[unit(s), lanes(h)] += r1[way, 2, unit(s)].astype(F32)

    def second(s, h, way, k):
        dx[unit_dx(s), lanes(h)] = own[unit(s), lanes(h)].astype(BF16)
        send(dx.at[unit_dx(s), lanes(h)], r2.at[way, k], two_s.at[way, k], two_r.at[way, k], q_dev[way])

    def add_two(s, h, way, k):
        arrived(r2.at[way, k], two_r.at[way, k])
        own[unit(s), lanes(h)] += r2[way, k].astype(F32)

    close_one(0)
    second(0, 1, 0, 0)
    second(0, 0, 1, 0)
    dw(1)
    close_one(1)
    second(1, 0, 0, 1)
    close_one(2)
    second(2, 1, 1, 1)
    dw(1)
    add_two(1, 1, 0, 0)
    second(1, 1, 0, 2)
    add_two(2, 0, 1, 0)
    second(2, 0, 1, 2)
    close_one(3)
    add_two(3, 0, 0, 1)
    add_two(3, 1, 1, 1)
    dw(1)
    release(0, (partner, *p_dev, *q_dev))
    add_two(3, 1, 0, 2)
    add_two(3, 0, 1, 2)
    dx[unit_dx(3), :] = own[unit(3), :].astype(BF16)

    uo = [q, wrap(q - 1), wrap(q + 1), wrap(q + 2)]
    go = [p, wrap(p - 1), wrap(p + 1), wrap(p + 2)]

    def piece(j, s, h=None):
        at = pl.ds(row_of(c, go[j], uo[s]), ur)
        return dx.at[at, :] if h is None else dx.at[at, lanes(h)]

    def spread(s):
        for way in range(2):
            send(piece(0, s), piece(0, s), ag1_s.at[way, s], ag1_r.at[way, s], p_dev[way])

    def share(j, s):
        send(piece(j, s), piece(j, s), agp_s.at[j, s], agp_r.at[j, s], partner)

    def relay(s):
        for way, h in ((0, 1), (1, 0)):
            arrived(piece(1 + way, s), ag1_r.at[way, s])
            send(piece(1 + way, s, h), piece(1 + way, s, h), ag1_s.at[2 + way, s], ag1_r.at[2 + way, s], p_dev[way])
            share(1 + way, s)

    def finish(s):
        for way, h in ((0, 1), (1, 0)):
            arrived(piece(3, s, h), ag1_r.at[2 + way, s])
        share(3, s)

    pl.semaphore_wait(free.at[0], 5)
    for way in range(2):
        send(piece(0, 0), piece(0, 0), ag2_s.at[way], ag2_r.at[way], q_dev[way])
    spread(0)
    share(0, 0)
    dw(2)
    for way, h in ((0, 1), (1, 0)):
        arrived(piece(0, 1 + way), ag2_r.at[way])
        send(piece(0, 1 + way, h), piece(0, 1 + way, h), ag2_s.at[2 + way], ag2_r.at[2 + way], q_dev[way])
        spread(1 + way)
        share(0, 1 + way)
    relay(0)
    dw(1)
    for way, h in ((0, 1), (1, 0)):
        arrived(piece(0, 3, h), ag2_r.at[2 + way])
    spread(3)
    share(0, 3)
    dw(2)
    relay(1)
    finish(0)
    dw(2)
    relay(2)
    finish(1)
    dw(STEPS)
    relay(3)
    finish(2)
    finish(3)
    for j in range(side):
        for s in range(side):
            arrived(piece(j, s), agp_r.at[j, s])
    for d in sent:
        d.wait_send()


def put_out(*refs):
    copies = [pltpu.make_async_copy(refs[i], refs[4 + i], refs[8].at[i]) for i in range(4)]
    for d in copies:
        d.start()
    for d in copies:
        d.wait()


def solution(mesh):
    tp = mesh.shape["tp"]
    side = math.isqrt(tp // 2)
    assert side == 4 and 2 * side * side == tp

    def step(x, dy, gate, up, w_gate, w_up, w_down):
        rows, width = x.shape
        f = gate.shape[1]
        gr, ur, cb, hw = rows // 8, rows // 32, width // STEPS, width // 2
        dma = pltpu.SemaphoreType.DMA
        out = lambda *s: pltpu.VMEM(s, BF16)
        flops = 12 * rows * width * f
        held = pl.pallas_call(
            functools.partial(kernel, side),
            out_shape=(out(rows, width), out(width, f), out(width, f), out(f, width)),
            in_specs=[pl.BlockSpec(memory_space=pl.ANY)] * 7,
            out_specs=[pl.BlockSpec(memory_space=pltpu.VMEM)] * 4,
            scratch_shapes=[
                pltpu.VMEM((f, width), BF16),
                pltpu.VMEM((width, 2 * f), BF16),
                pltpu.VMEM((2, gr, f), BF16),
                pltpu.VMEM((2, gr, f), BF16),
                pltpu.VMEM((2, gr, width), BF16),
                pltpu.VMEM((rows, 2 * f), BF16),
                pltpu.VMEM((f, rows), BF16),
                pltpu.VMEM((2, 3, gr, hw), BF16),
                pltpu.VMEM((2, 3, ur, hw), BF16),
                pltpu.VMEM((gr, width), F32),
                pltpu.VMEM((2, rows, cb), BF16),
                pltpu.VMEM((2, rows, cb), BF16),
                dma((3,)),
                dma((2, 3)),
                dma((2, 2)),
                pltpu.SemaphoreType.REGULAR((1,)),
                dma((4, 2)), dma((4, 2)),
                dma((2, 6)), dma((2, 6)),
                dma((2, 3)), dma((2, 3)),
                dma((4,)), dma((4,)),
                dma((4, 4)), dma((4, 4)),
                dma((4, 4)), dma((4, 4)),
            ],
            compiler_params=pltpu.CompilerParams(
                collective_id=0, has_side_effects=True, vmem_limit_bytes=VMEM_LIMIT
            ),
            cost_estimate=pl.CostEstimate(flops=flops, bytes_accessed=80 * MIB, transcendentals=rows * f),
        )(x, dy, gate, up, w_gate, w_up, w_down)
        return pl.pallas_call(
            put_out,
            out_shape=tuple(jax.ShapeDtypeStruct(h.shape, h.dtype) for h in held),
            in_specs=[pl.BlockSpec(memory_space=pltpu.VMEM)] * 4,
            out_specs=[pl.BlockSpec(memory_space=pltpu.HBM)] * 4,
            scratch_shapes=[dma((4,))],
            compiler_params=pltpu.CompilerParams(vmem_limit_bytes=2 * MIB),
        )(*held)

    tokens, columns, rows = P("dp", None), P(None, "tp"), P("tp", None)
    return jax.shard_map(
        step,
        mesh=mesh,
        in_specs=(tokens, tokens, P("dp", "tp"), P("dp", "tp"), columns, columns, rows),
        out_specs=(tokens, P("dp", "tp"), P("dp", "tp"), P(("dp", "tp"), None)),
        check_vma=False,
    )


VMEM_LIMIT = 37 * MIB
```

```python
import functools
import math

import jax
import jax.numpy as jnp
from jax import lax
from jax.experimental import pallas as pl
from jax.experimental.pallas import tpu as pltpu
from jax.sharding import PartitionSpec as P

F32, BF16 = jnp.float32, jnp.bfloat16
STEPS = 16
PARTS = 4
MIB = 1 << 20


def contract(a, b, ca, cb):
    return lax.dot_general(a, b, (((ca,), (cb,)), ((), ())), preferred_element_type=F32)


def kernel(
    side,
    x_hbm, dy_hbm, gate_hbm, up_hbm, wg_hbm, wu_hbm, wd_hbm,
    dx, dwg, dwu, dwd,
    wd_v, wc_v, gate_v, up_v, row_v, dc_v, ht_v, r1, r2, own, xcol_v, dycol_v,
    w_sem, row_sem, col_sem,
    free, pair_s, pair_r, one_s, one_r, two_s, two_r, ag2_s, ag2_r, ag1_s, ag1_r, agp_s, agp_r,
):
    rows, width = dx.shape
    f = wd_v.shape[0]
    half, hw = rows // 2, width // 2
    gr = half // side
    ur = gr // side
    cb = width // STEPS

    me = lax.axis_index("tp")
    c = lax.rem(me, 2)
    chip = lax.div(me, 2)
    cx, cy = lax.div(chip, side), lax.rem(chip, side)
    p = cx * (1 - c) + cy * c
    q = cy * (1 - c) + cx * c

    def wrap(v):
        return lax.rem(v + side, side)

    def device(pp, qq, cc):
        return {"tp": ((pp * (1 - cc) + qq * cc) * side + (qq * (1 - cc) + pp * cc)) * 2 + cc}

    partner = {"tp": chip * 2 + (1 - c)}
    p_dev = (device(wrap(p + 1), q, c), device(wrap(p - 1), q, c))
    q_dev = (device(p, wrap(q + 1), c), device(p, wrap(q - 1), c))
    offs = (2, 1, -1, 0)
    pg = [wrap(p + o) for o in offs]
    qg = [wrap(q + o) for o in offs]

    def row_of(cc, g, u):
        return pl.multiple_of(cc * half + g * gr + u * ur, ur)

    def remote(src, dst, s, r, dev):
        return pltpu.make_async_remote_copy(
            src_ref=src, dst_ref=dst, send_sem=s, recv_sem=r, device_id=dev, device_id_type=pl.DeviceIdType.MESH
        )

    def arrived(ref, r):
        remote(ref, ref, r, r, partner).wait_recv()

    def left(ref, s):
        remote(ref, ref, s, s, partner).wait_send()

    qw = width // 4

    def lanes(w, h):
        return pl.ds(pl.multiple_of(w * hw + h * qw, qw), qw)

    def whole(w):
        return pl.ds(w * hw, hw)

    w_copies = [
        pltpu.make_async_copy(wd_hbm, wd_v, w_sem.at[0]),
        pltpu.make_async_copy(wg_hbm, wc_v.at[:, pl.ds(0, f)], w_sem.at[1]),
        pltpu.make_async_copy(wu_hbm, wc_v.at[:, pl.ds(f, f)], w_sem.at[2]),
    ]
    order = [(1 - c, qg[0]), (c, pg[0]), (1 - c, qg[1]), (1 - c, qg[2]), (c, pg[1]), (c, pg[2]), (1 - c, qg[3]), (c, pg[3])]

    def row_copies(i):
        at = pl.ds(row_of(*order[i], 0), gr)
        slot = i % 2
        return [
            pltpu.make_async_copy(dy_hbm.at[at, :], row_v.at[slot], row_sem.at[slot, 0]),
            pltpu.make_async_copy(gate_hbm.at[at, :], gate_v.at[slot], row_sem.at[slot, 1]),
            pltpu.make_async_copy(up_hbm.at[at, :], up_v.at[slot], row_sem.at[slot, 2]),
        ]

    def col_copies(i, slot):
        at = pl.ds(pl.multiple_of(i * cb, cb), cb)
        return [
            pltpu.make_async_copy(x_hbm.at[:, at], xcol_v.at[slot], col_sem.at[slot, 0]),
            pltpu.make_async_copy(dy_hbm.at[:, at], dycol_v.at[slot], col_sem.at[slot, 1]),
        ]

    w_copies[0].start()
    for d in row_copies(0):
        d.start()
    for d in w_copies[1:]:
        d.start()

    barrier = pltpu.get_barrier_semaphore()
    for dev in (partner, *p_dev, *q_dev):
        pl.semaphore_signal(barrier, inc=1, device_id=dev, device_id_type=pl.DeviceIdType.MESH)

    w_copies[0].wait()

    def hidden(i):
        slot = i % 2
        if i + 1 < len(order):
            for d in row_copies(i + 1):
                d.start()
        for d in row_copies(i):
            d.wait()
        dh = contract(row_v[slot], wd_v[...], 1, 1)
        g, u = gate_v[slot].astype(F32), up_v[slot].astype(F32)
        s = jax.nn.sigmoid(g)
        silu = g * s
        at = pl.ds(row_of(*order[i], 0), gr)
        dc_v[at, pl.ds(0, f)] = (dh * u * (s + silu * (1.0 - s))).astype(BF16)
        dc_v[at, pl.ds(f, f)] = (dh * silu).astype(BF16)
        ht_v[:, pl.ds(pl.multiple_of(row_of(*order[i], 0), gr), gr)] = (silu * u).astype(BF16).T

    def term(row, w, h):
        return contract(dc_v[pl.ds(row, gr), :], wc_v[lanes(w, h), :], 1, 1)

    def piece_of(row, w, h):
        return dx.at[pl.ds(row, gr), lanes(w, h)]

    def to_partner(k, w):
        row = row_of(1 - c, qg[k], 0)

        @pl.loop(0, 2)
        def _(h):
            part = piece_of(row, w, h)
            part[...] = term(row, w, h).astype(BF16)
            remote(part, part, pair_s.at[w, k, h], pair_r.at[w, k, h], partner).start()

    def with_partner(k, w, h, row):
        part = piece_of(row, w, h)
        arrived(part, pair_r.at[w, k, h])
        return part, term(row, w, h) + part[...].astype(F32)

    def p_at(way):
        return {"tp": p_dev[0]["tp"] * (1 - way) + p_dev[1]["tp"] * way}

    def first_far(w):
        row = row_of(c, pg[0], 0)

        @pl.loop(0, 2)
        def _(way):
            part, t = with_partner(0, w, 1 - way, row)
            part[...] = t.astype(BF16)
            remote(part, r1.at[w, way, 0], one_s.at[w, way, 0], one_r.at[w, way, 0], p_at(way)).start()

    def first_near(w):
        @pl.loop(0, 2)
        def _(way):
            row = row_of(c, pg[1] * (1 - way) + pg[2] * way, 0)
            part, t = with_partner(1 + way, w, way, row)
            part[...] = t.astype(BF16)
            remote(part, r1.at[w, way, 1], one_s.at[w, way, 1], one_r.at[w, way, 1], p_at(way)).start()

    def first_joined(w):
        @pl.loop(0, 2)
        def _(way):
            row = row_of(c, pg[1] * (1 - way) + pg[2] * way, 0)
            part, t = with_partner(1 + way, w, 1 - way, row)
            arrived(r1.at[w, way, 0], one_r.at[w, way, 0])
            part[...] = (t + r1[w, way, 0].astype(F32)).astype(BF16)
            for s in range(side):
                at = unit(s)
                to = r1.at[w, way, 2, at]
                remote(part.at[at], to, one_s.at[w, way, 2 + s], one_r.at[w, way, 2 + s], p_at(way)).start()

    def first_own(w):
        @pl.loop(0, 2)
        def _(h):
            _, t = with_partner(3, w, h, row_of(c, pg[3], 0))
            own[:, lanes(w, h)] = t

    def unit(s):
        return pl.ds(pl.multiple_of(qg[s] * ur, ur), ur)

    def dw_block(i):
        slot = lax.rem(i, 2)

        @pl.when(i + 1 < STEPS)
        def _():
            for d in col_copies(i + 1, 1 - slot):
                d.start()

        for d in col_copies(i, slot):
            d.wait()
        at = pl.ds(pl.multiple_of(i * cb, cb), cb)
        both = contract(xcol_v[slot], dc_v[...], 0, 0).astype(BF16)
        dwg[at, :] = both[:, :f]
        dwu[at, :] = both[:, f:]
        dwd[:, at] = jnp.dot(ht_v[...], dycol_v[slot], preferred_element_type=F32).astype(BF16)

    done = [0]

    def dw(n):
        lo = done[0]
        done[0] = min(STEPS, lo + n)
        pl.loop(lo, done[0])(dw_block)

    def first_in(w):
        for h in range(2):
            arrived(r1.at[w, h, 1], one_r.at[w, h, 1])
            own[:, lanes(w, h)] += r1[w, h, 1].astype(F32)

    def unit_dx(s):
        return pl.ds(row_of(c, p, qg[s]), ur)

    def close_one(s, w):
        for h, way in ((1, 0), (0, 1)):
            arrived(r1.at[w, way, 2, unit(s)], one_r.at[w, way, 2 + s])
            own[unit(s), lanes(w, h)] += r1[w, way, 2, unit(s)].astype(F32)

    def second(s, w, h, way, k):
        part = dx.at[unit_dx(s), lanes(w, h)]
        part[...] = own[unit(s), lanes(w, h)].astype(BF16)
        remote(part, r2.at[w, way, k], two_s.at[w, way, k], two_r.at[w, way, k], q_dev[way]).start()

    def add_two(s, w, h, way, k):
        arrived(r2.at[w, way, k], two_r.at[w, way, k])
        own[unit(s), lanes(w, h)] += r2[w, way, k].astype(F32)

    def second_far(w):
        close_one(0, w)
        second(0, w, 1, 0, 0)
        second(0, w, 0, 1, 0)

    def second_near(w):
        close_one(1, w)
        second(1, w, 0, 0, 1)
        close_one(2, w)
        second(2, w, 1, 1, 1)

    def second_joined(w):
        add_two(1, w, 1, 0, 0)
        second(1, w, 1, 0, 2)
        add_two(2, w, 0, 1, 0)
        second(2, w, 0, 1, 2)

    def second_own(w):
        close_one(3, w)
        add_two(3, w, 0, 0, 1)
        add_two(3, w, 1, 1, 1)

    def close(w):
        add_two(3, w, 1, 0, 2)
        add_two(3, w, 0, 1, 2)
        dx[unit_dx(3), whole(w)] = own[unit(3), whole(w)].astype(BF16)

    def release(w):
        for k in range(side):
            for h in range(2):
                left(piece_of(row_of(1 - c, qg[k], 0), w, h), pair_s.at[w, k, h])
        for way in range(2):
            for k in range(2):
                left(r1.at[w, way, k], one_s.at[w, way, k])
            for s in range(side):
                left(r1.at[w, way, 2, unit(s)], one_s.at[w, way, 2 + s])
            for k in range(3):
                left(r2.at[w, way, k], two_s.at[w, way, k])
        for dev in (partner, *p_dev, *q_dev):
            pl.semaphore_signal(free.at[w], inc=1, device_id=dev, device_id_type=pl.DeviceIdType.MESH)

    uo = [q, wrap(q - 1), wrap(q + 1), wrap(q + 2)]
    go = [p, wrap(p - 1), wrap(p + 1), wrap(p + 2)]
    sent = []

    def send(src, s, r, dev):
        d = remote(src, src, s, r, dev)
        d.start()
        sent.append(d)

    def piece(j, s, w, h=None):
        return dx.at[pl.ds(row_of(c, go[j], uo[s]), ur), whole(w) if h is None else lanes(w, h)]

    def spread(s, w):
        for way in range(2):
            send(piece(0, s, w), ag1_s.at[w, way, s], ag1_r.at[w, way, s], p_dev[way])

    def share(j, s, w):
        send(piece(j, s, w), agp_s.at[w, j, s], agp_r.at[w, j, s], partner)

    def open_gather(w):
        pl.semaphore_wait(free.at[w], 5)
        for way in range(2):
            send(piece(0, 0, w), ag2_s.at[w, way], ag2_r.at[w, way], q_dev[way])
        spread(0, w)
        share(0, 0, w)

    def gather_near(w):
        for way, h in ((0, 1), (1, 0)):
            arrived(piece(0, 1 + way, w), ag2_r.at[w, way])
            send(piece(0, 1 + way, w, h), ag2_s.at[w, 2 + way], ag2_r.at[w, 2 + way], q_dev[way])
            spread(1 + way, w)
            share(0, 1 + way, w)

    def gather_far(w):
        for way, h in ((0, 1), (1, 0)):
            arrived(piece(0, 3, w, h), ag2_r.at[w, 2 + way])
        spread(3, w)
        share(0, 3, w)

    def relay(s, w):
        for way, h in ((0, 1), (1, 0)):
            arrived(piece(1 + way, s, w), ag1_r.at[w, way, s])
            send(piece(1 + way, s, w, h), ag1_s.at[w, 2 + way, s], ag1_r.at[w, 2 + way, s], p_dev[way])
            share(1 + way, s, w)

    def finish(s, w):
        for way, h in ((0, 1), (1, 0)):
            arrived(piece(3, s, w, h), ag1_r.at[w, 2 + way, s])
        share(3, s, w)

    hidden(0)
    for d in w_copies[1:]:
        d.wait()
    pl.semaphore_wait(barrier, 5)
    to_partner(0, 0)
    hidden(1)
    first_far(0)
    hidden(2)
    to_partner(1, 0)
    hidden(3)
    to_partner(2, 0)
    hidden(4)
    hidden(5)
    first_near(0)
    to_partner(0, 1)
    first_joined(0)
    hidden(6)
    to_partner(3, 0)
    hidden(7)
    for d in col_copies(0, 0):
        d.start()
    first_own(0)
    first_far(1)
    to_partner(1, 1)
    to_partner(2, 1)
    first_near(1)
    first_in(0)
    second_far(0)
    to_partner(3, 1)
    first_own(1)
    second_near(0)
    dw(2)
    second_joined(0)
    second_own(0)
    dw(2)
    first_joined(1)
    close(0)
    release(0)
    dw(1)
    open_gather(0)
    first_in(1)
    dw(2)
    second_far(1)
    second_near(1)
    gather_near(0)
    second_joined(1)
    relay(0, 0)
    second_own(1)
    gather_far(0)
    close(1)
    release(1)
    dw(2)
    open_gather(1)
    relay(1, 0)
    finish(0, 0)
    relay(2, 0)
    dw(2)
    gather_near(1)
    finish(1, 0)
    relay(3, 0)
    finish(2, 0)
    relay(0, 1)
    finish(3, 0)
    dw(2)
    gather_far(1)
    relay(1, 1)
    finish(0, 1)
    dw(STEPS)
    relay(2, 1)
    finish(1, 1)
    relay(3, 1)
    finish(2, 1)
    finish(3, 1)
    for w in range(2):
        for j in range(side):
            for s in range(side):
                arrived(piece(j, s, w), agp_r.at[w, j, s])
    for d in sent:
        d.wait_send()


def put_out(*refs):
    copies = []
    for i in range(4):
        rows = refs[i].shape[0] // PARTS
        for k in range(PARTS):
            at = pl.ds(k * rows, rows)
            copies.append(pltpu.make_async_copy(refs[i].at[at], refs[4 + i].at[at], refs[8].at[i, k]))
    for d in copies:
        d.start()
    for d in copies:
        d.wait()


def solution(mesh):
    tp = mesh.shape["tp"]
    side = math.isqrt(tp // 2)
    assert side == 4 and 2 * side * side == tp

    def step(x, dy, gate, up, w_gate, w_up, w_down):
        rows, width = x.shape
        f = gate.shape[1]
        gr, ur, cb, qw = rows // 8, rows // 32, width // STEPS, width // 4
        dma = pltpu.SemaphoreType.DMA
        out = lambda *s: pltpu.VMEM(s, BF16)
        flops = 12 * rows * width * f
        held = pl.pallas_call(
            functools.partial(kernel, side),
            out_shape=(out(rows, width), out(width, f), out(width, f), out(f, width)),
            in_specs=[pl.BlockSpec(memory_space=pl.ANY)] * 7,
            out_specs=[pl.BlockSpec(memory_space=pltpu.VMEM)] * 4,
            scratch_shapes=[
                pltpu.VMEM((f, width), BF16),
                pltpu.VMEM((width, 2 * f), BF16),
                pltpu.VMEM((2, gr, f), BF16),
                pltpu.VMEM((2, gr, f), BF16),
                pltpu.VMEM((2, gr, width), BF16),
                pltpu.VMEM((rows, 2 * f), BF16),
                pltpu.VMEM((f, rows), BF16),
                pltpu.VMEM((2, 2, 3, gr, qw), BF16),
                pltpu.VMEM((2, 2, 3, ur, qw), BF16),
                pltpu.VMEM((gr, width), F32),
                pltpu.VMEM((2, rows, cb), BF16),
                pltpu.VMEM((2, rows, cb), BF16),
                dma((3,)),
                dma((2, 3)),
                dma((2, 2)),
                pltpu.SemaphoreType.REGULAR((2,)),
                dma((2, 4, 2)), dma((2, 4, 2)),
                dma((2, 2, 6)), dma((2, 2, 6)),
                dma((2, 2, 3)), dma((2, 2, 3)),
                dma((2, 4)), dma((2, 4)),
                dma((2, 4, 4)), dma((2, 4, 4)),
                dma((2, 4, 4)), dma((2, 4, 4)),
            ],
            compiler_params=pltpu.CompilerParams(
                collective_id=0, has_side_effects=True, vmem_limit_bytes=VMEM_LIMIT
            ),
            cost_estimate=pl.CostEstimate(flops=flops, bytes_accessed=80 * MIB, transcendentals=rows * f),
        )(x, dy, gate, up, w_gate, w_up, w_down)
        return pl.pallas_call(
            put_out,
            out_shape=tuple(jax.ShapeDtypeStruct(h.shape, h.dtype) for h in held),
            in_specs=[pl.BlockSpec(memory_space=pltpu.VMEM)] * 4,
            out_specs=[pl.BlockSpec(memory_space=pltpu.HBM)] * 4,
            scratch_shapes=[dma((4, PARTS))],
            compiler_params=pltpu.CompilerParams(vmem_limit_bytes=2 * MIB),
        )(*held)

    tokens, columns, rows = P("dp", None), P(None, "tp"), P("tp", None)
    return jax.shard_map(
        step,
        mesh=mesh,
        in_specs=(tokens, tokens, P("dp", "tp"), P("dp", "tp"), columns, columns, rows),
        out_specs=(tokens, P("dp", "tp"), P("dp", "tp"), P(("dp", "tp"), None)),
        check_vma=False,
    )


VMEM_LIMIT = 37 * MIB
```

```python
import functools
import math

import jax
import jax.numpy as jnp
from jax import lax
from jax.experimental import pallas as pl
from jax.experimental.pallas import tpu as pltpu
from jax.sharding import PartitionSpec as P

F32, BF16 = jnp.float32, jnp.bfloat16
STEPS = 16
PARTS = 4
MIB = 1 << 20


def contract(a, b, ca, cb):
    return lax.dot_general(a, b, (((ca,), (cb,)), ((), ())), preferred_element_type=F32)


def kernel(
    side,
    x_hbm, dy_hbm, gate_hbm, up_hbm, wg_hbm, wu_hbm, wd_hbm,
    dx, dwg, dwu, dwd,
    wd_v, wc_v, gate_v, up_v, row_v, dc_v, ht_v, r1, r2, own, xcol_v, dycol_v,
    w_sem, row_sem, col_sem,
    free, pair_s, pair_r, one_s, one_r, two_s, two_r, ag2_s, ag2_r, ag1_s, ag1_r, agp_s, agp_r,
):
    rows, width = dx.shape
    f = wd_v.shape[0]
    half, hw = rows // 2, width // 2
    gr = half // side
    ur = gr // side
    cb = width // STEPS

    me = lax.axis_index("tp")
    c = lax.rem(me, 2)
    chip = lax.div(me, 2)
    cx, cy = lax.div(chip, side), lax.rem(chip, side)
    p = cx * (1 - c) + cy * c
    q = cy * (1 - c) + cx * c

    def wrap(v):
        return lax.rem(v + side, side)

    def device(pp, qq, cc):
        return {"tp": ((pp * (1 - cc) + qq * cc) * side + (qq * (1 - cc) + pp * cc)) * 2 + cc}

    partner = {"tp": chip * 2 + (1 - c)}
    p_dev = (device(wrap(p + 1), q, c), device(wrap(p - 1), q, c))
    q_dev = (device(p, wrap(q + 1), c), device(p, wrap(q - 1), c))
    offs = (2, 1, -1, 0)
    pg = [wrap(p + o) for o in offs]
    qg = [wrap(q + o) for o in offs]

    def row_of(cc, g, u):
        return pl.multiple_of(cc * half + g * gr + u * ur, ur)

    def remote(src, dst, s, r, dev):
        return pltpu.make_async_remote_copy(
            src_ref=src, dst_ref=dst, send_sem=s, recv_sem=r, device_id=dev, device_id_type=pl.DeviceIdType.MESH
        )

    def arrived(ref, r):
        remote(ref, ref, r, r, partner).wait_recv()

    def left(ref, s):
        remote(ref, ref, s, s, partner).wait_send()

    qw = width // 4

    def lanes(w, h):
        return pl.ds(pl.multiple_of(w * hw + h * qw, qw), qw)

    def whole(w):
        return pl.ds(w * hw, hw)

    w_copies = [pltpu.make_async_copy(wd_hbm, wd_v, w_sem.at[0])]
    for w in range(2):
        at = pl.ds(w * hw, hw)
        w_copies += [
            pltpu.make_async_copy(wg_hbm.at[at, :], wc_v.at[at, pl.ds(0, f)], w_sem.at[1 + 2 * w]),
            pltpu.make_async_copy(wu_hbm.at[at, :], wc_v.at[at, pl.ds(f, f)], w_sem.at[2 + 2 * w]),
        ]
    order = [(1 - c, qg[0]), (c, pg[0]), (1 - c, qg[1]), (1 - c, qg[2]), (c, pg[1]), (c, pg[2]), (1 - c, qg[3]), (c, pg[3])]

    def row_copies(i):
        at = pl.ds(row_of(*order[i], 0), gr)
        slot = i % 2
        return [
            pltpu.make_async_copy(dy_hbm.at[at, :], row_v.at[slot], row_sem.at[slot, 0]),
            pltpu.make_async_copy(gate_hbm.at[at, :], gate_v.at[slot], row_sem.at[slot, 1]),
            pltpu.make_async_copy(up_hbm.at[at, :], up_v.at[slot], row_sem.at[slot, 2]),
        ]

    def col_copies(i, slot):
        at = pl.ds(pl.multiple_of(i * cb, cb), cb)
        return [
            pltpu.make_async_copy(x_hbm.at[:, at], xcol_v.at[slot], col_sem.at[slot, 0]),
            pltpu.make_async_copy(dy_hbm.at[:, at], dycol_v.at[slot], col_sem.at[slot, 1]),
        ]

    w_copies[0].start()
    for d in row_copies(0):
        d.start()
    for d in w_copies[1:3]:
        d.start()

    barrier = pltpu.get_barrier_semaphore()
    for dev in (partner, *p_dev, *q_dev):
        pl.semaphore_signal(barrier, inc=1, device_id=dev, device_id_type=pl.DeviceIdType.MESH)

    w_copies[0].wait()

    def hidden(i):
        slot = i % 2
        if i + 1 < len(order):
            for d in row_copies(i + 1):
                d.start()
        for d in row_copies(i):
            d.wait()
        dh = contract(row_v[slot], wd_v[...], 1, 1)
        g, u = gate_v[slot].astype(F32), up_v[slot].astype(F32)
        s = jax.nn.sigmoid(g)
        silu = g * s
        at = pl.ds(row_of(*order[i], 0), gr)
        dc_v[at, pl.ds(0, f)] = (dh * u * (s + silu * (1.0 - s))).astype(BF16)
        dc_v[at, pl.ds(f, f)] = (dh * silu).astype(BF16)
        ht_v[:, pl.ds(pl.multiple_of(row_of(*order[i], 0), gr), gr)] = (silu * u).astype(BF16).T

    def term(row, w, h):
        return contract(dc_v[pl.ds(row, gr), :], wc_v[lanes(w, h), :], 1, 1)

    def piece_of(row, w, h):
        return dx.at[pl.ds(row, gr), lanes(w, h)]

    def to_partner(k, w):
        row = row_of(1 - c, qg[k], 0)

        @pl.loop(0, 2)
        def _(h):
            part = piece_of(row, w, h)
            part[...] = term(row, w, h).astype(BF16)
            remote(part, part, pair_s.at[w, k, h], pair_r.at[w, k, h], partner).start()

    def with_partner(k, w, h, row):
        part = piece_of(row, w, h)
        arrived(part, pair_r.at[w, k, h])
        return part, term(row, w, h) + part[...].astype(F32)

    def p_at(way):
        return {"tp": p_dev[0]["tp"] * (1 - way) + p_dev[1]["tp"] * way}

    def first_far(w):
        row = row_of(c, pg[0], 0)

        @pl.loop(0, 2)
        def _(h):
            way = 1 - h
            part, t = with_partner(0, w, h, row)
            part[...] = t.astype(BF16)
            remote(part, r1.at[w, way, 0], one_s.at[w, way, 0], one_r.at[w, way, 0], p_at(way)).start()

    def first_near(w):
        @pl.loop(0, 2)
        def _(way):
            row = row_of(c, pg[1] * (1 - way) + pg[2] * way, 0)
            part, t = with_partner(1 + way, w, way, row)
            part[...] = t.astype(BF16)
            remote(part, r1.at[w, way, 1], one_s.at[w, way, 1], one_r.at[w, way, 1], p_at(way)).start()

    def first_joined(w):
        @pl.loop(0, 2)
        def _(way):
            row = row_of(c, pg[1] * (1 - way) + pg[2] * way, 0)
            part, t = with_partner(1 + way, w, 1 - way, row)
            arrived(r1.at[w, way, 0], one_r.at[w, way, 0])
            part[...] = (t + r1[w, way, 0].astype(F32)).astype(BF16)
            for s in range(side):
                at = unit(s)
                to = r1.at[w, way, 2, at]
                remote(part.at[at], to, one_s.at[w, way, 2 + s], one_r.at[w, way, 2 + s], p_at(way)).start()

    def first_own(w):
        @pl.loop(0, 2)
        def _(h):
            _, t = with_partner(3, w, h, row_of(c, pg[3], 0))
            own[:, lanes(w, h)] = t

    def unit(s):
        return pl.ds(pl.multiple_of(qg[s] * ur, ur), ur)

    def dw_block(i):
        slot = lax.rem(i, 2)

        @pl.when(i + 1 < STEPS)
        def _():
            for d in col_copies(i + 1, 1 - slot):
                d.start()

        for d in col_copies(i, slot):
            d.wait()
        at = pl.ds(pl.multiple_of(i * cb, cb), cb)
        both = contract(xcol_v[slot], dc_v[...], 0, 0).astype(BF16)
        dwg[at, :] = both[:, :f]
        dwu[at, :] = both[:, f:]
        dwd[:, at] = jnp.dot(ht_v[...], dycol_v[slot], preferred_element_type=F32).astype(BF16)

    done = [0]

    def dw(n):
        lo = done[0]
        done[0] = min(STEPS, lo + n)
        pl.loop(lo, done[0])(dw_block)

    def first_in(w):
        for h in range(2):
            arrived(r1.at[w, h, 1], one_r.at[w, h, 1])
            own[:, lanes(w, h)] += r1[w, h, 1].astype(F32)

    def unit_dx(s):
        return pl.ds(row_of(c, p, qg[s]), ur)

    def close_one(s, w):
        for h, way in ((1, 0), (0, 1)):
            arrived(r1.at[w, way, 2, unit(s)], one_r.at[w, way, 2 + s])
            own[unit(s), lanes(w, h)] += r1[w, way, 2, unit(s)].astype(F32)

    def second(s, w, h, way, k):
        part = dx.at[unit_dx(s), lanes(w, h)]
        part[...] = own[unit(s), lanes(w, h)].astype(BF16)
        remote(part, r2.at[w, way, k], two_s.at[w, way, k], two_r.at[w, way, k], q_dev[way]).start()

    def add_two(s, w, h, way, k):
        arrived(r2.at[w, way, k], two_r.at[w, way, k])
        own[unit(s), lanes(w, h)] += r2[w, way, k].astype(F32)

    def second_far(w):
        close_one(0, w)
        second(0, w, 1, 0, 0)
        second(0, w, 0, 1, 0)

    def second_near(w):
        close_one(1, w)
        second(1, w, 0, 0, 1)
        close_one(2, w)
        second(2, w, 1, 1, 1)

    def second_joined(way, w):
        add_two(1 + way, w, 1 - way, way, 0)
        second(1 + way, w, 1 - way, way, 2)

    def second_own(w):
        close_one(3, w)
        add_two(3, w, 0, 0, 1)
        add_two(3, w, 1, 1, 1)

    def close(w):
        add_two(3, w, 1, 0, 2)
        add_two(3, w, 0, 1, 2)
        dx[unit_dx(3), whole(w)] = own[unit(3), whole(w)].astype(BF16)

    def release(w):
        for k in range(side):
            for h in range(2):
                left(piece_of(row_of(1 - c, qg[k], 0), w, h), pair_s.at[w, k, h])
        for way in range(2):
            for k in range(2):
                left(r1.at[w, way, k], one_s.at[w, way, k])
            for s in range(side):
                left(r1.at[w, way, 2, unit(s)], one_s.at[w, way, 2 + s])
            for k in range(3):
                left(r2.at[w, way, k], two_s.at[w, way, k])
        for dev in (partner, *p_dev, *q_dev):
            pl.semaphore_signal(free.at[w], inc=1, device_id=dev, device_id_type=pl.DeviceIdType.MESH)

    uo = [q, wrap(q - 1), wrap(q + 1), wrap(q + 2)]
    go = [p, wrap(p - 1), wrap(p + 1), wrap(p + 2)]
    sent = []

    def send(src, s, r, dev):
        d = remote(src, src, s, r, dev)
        d.start()
        sent.append(d)

    def piece(j, s, w, h=None):
        return dx.at[pl.ds(row_of(c, go[j], uo[s]), ur), whole(w) if h is None else lanes(w, h)]

    def spread(s, w):
        for way in range(2):
            send(piece(0, s, w), ag1_s.at[w, way, s], ag1_r.at[w, way, s], p_dev[way])

    def share(j, s, w):
        send(piece(j, s, w), agp_s.at[w, j, s], agp_r.at[w, j, s], partner)

    def open_gather(w):
        pl.semaphore_wait(free.at[w], 5)
        for way in range(2):
            send(piece(0, 0, w), ag2_s.at[w, way], ag2_r.at[w, way], q_dev[way])
        spread(0, w)
        share(0, 0, w)

    def gather_near(way, w):
        arrived(piece(0, 1 + way, w), ag2_r.at[w, way])
        send(piece(0, 1 + way, w, 1 - way), ag2_s.at[w, 2 + way], ag2_r.at[w, 2 + way], q_dev[way])
        spread(1 + way, w)
        share(0, 1 + way, w)

    def gather_far(w):
        for way, h in ((0, 1), (1, 0)):
            arrived(piece(0, 3, w, h), ag2_r.at[w, 2 + way])
        spread(3, w)
        share(0, 3, w)

    def relay(way, s, w):
        arrived(piece(1 + way, s, w), ag1_r.at[w, way, s])
        send(piece(1 + way, s, w, 1 - way), ag1_s.at[w, 2 + way, s], ag1_r.at[w, 2 + way, s], p_dev[way])
        share(1 + way, s, w)

    def finish(s, w):
        for way, h in ((0, 1), (1, 0)):
            arrived(piece(3, s, w, h), ag1_r.at[w, 2 + way, s])
        share(3, s, w)

    hidden(0)
    for d in w_copies[3:]:
        d.start()
    for d in w_copies[1:3]:
        d.wait()
    pl.semaphore_wait(barrier, 5)
    to_partner(0, 0)
    hidden(1)
    first_far(0)
    hidden(2)
    to_partner(1, 0)
    hidden(3)
    to_partner(2, 0)
    hidden(4)
    hidden(5)
    hidden(6)
    first_near(0)
    to_partner(3, 0)
    hidden(7)
    for d in col_copies(0, 0):
        d.start()
    for d in w_copies[3:]:
        d.wait()
    to_partner(0, 1)
    first_joined(0)
    first_own(0)
    to_partner(1, 1)
    first_far(1)
    to_partner(2, 1)
    to_partner(3, 1)
    dw(1)
    first_in(0)
    dw(1)
    second_far(0)
    first_near(1)
    first_own(1)
    second_near(0)
    dw(3)
    second_joined(0, 0)
    second_joined(1, 0)
    dw(2)
    second_own(0)
    dw(3)
    close(0)
    release(0)
    dw(1)
    open_gather(0)
    first_joined(1)
    dw(5)
    first_in(1)
    gather_near(0, 0)
    gather_near(1, 0)
    relay(0, 0, 0)
    relay(1, 0, 0)
    gather_far(0)
    second_far(1)
    second_near(1)
    second_joined(0, 1)
    second_joined(1, 1)
    second_own(1)
    relay(0, 1, 0)
    relay(1, 1, 0)
    close(1)
    release(1)
    open_gather(1)
    relay(0, 2, 0)
    relay(1, 2, 0)
    finish(0, 0)
    gather_near(0, 1)
    gather_near(1, 1)
    relay(0, 3, 0)
    relay(1, 3, 0)
    finish(1, 0)
    gather_far(1)
    relay(0, 0, 1)
    relay(1, 0, 1)
    finish(2, 0)
    relay(0, 1, 1)
    relay(1, 1, 1)
    relay(0, 2, 1)
    relay(1, 2, 1)
    finish(3, 0)
    relay(0, 3, 1)
    relay(1, 3, 1)
    finish(0, 1)
    finish(1, 1)
    finish(2, 1)
    finish(3, 1)
    for w in range(2):
        for j in range(side):
            for s in range(side):
                arrived(piece(j, s, w), agp_r.at[w, j, s])
    for d in sent:
        d.wait_send()


def put_out(*refs):
    copies = []
    for i in range(4):
        rows = refs[i].shape[0] // PARTS
        for k in range(PARTS):
            at = pl.ds(k * rows, rows)
            copies.append(pltpu.make_async_copy(refs[i].at[at], refs[4 + i].at[at], refs[8].at[i, k]))
    for d in copies:
        d.start()
    for d in copies:
        d.wait()


def solution(mesh):
    tp = mesh.shape["tp"]
    side = math.isqrt(tp // 2)
    assert side == 4 and 2 * side * side == tp

    def step(x, dy, gate, up, w_gate, w_up, w_down):
        rows, width = x.shape
        f = gate.shape[1]
        gr, ur, cb, qw = rows // 8, rows // 32, width // STEPS, width // 4
        dma = pltpu.SemaphoreType.DMA
        out = lambda *s: pltpu.VMEM(s, BF16)
        flops = 12 * rows * width * f
        held = pl.pallas_call(
            functools.partial(kernel, side),
            out_shape=(out(rows, width), out(width, f), out(width, f), out(f, width)),
            in_specs=[pl.BlockSpec(memory_space=pl.ANY)] * 7,
            out_specs=[pl.BlockSpec(memory_space=pltpu.VMEM)] * 4,
            scratch_shapes=[
                pltpu.VMEM((f, width), BF16),
                pltpu.VMEM((width, 2 * f), BF16),
                pltpu.VMEM((2, gr, f), BF16),
                pltpu.VMEM((2, gr, f), BF16),
                pltpu.VMEM((2, gr, width), BF16),
                pltpu.VMEM((rows, 2 * f), BF16),
                pltpu.VMEM((f, rows), BF16),
                pltpu.VMEM((2, 2, 3, gr, qw), BF16),
                pltpu.VMEM((2, 2, 3, ur, qw), BF16),
                pltpu.VMEM((gr, width), F32),
                pltpu.VMEM((2, rows, cb), BF16),
                pltpu.VMEM((2, rows, cb), BF16),
                dma((5,)),
                dma((2, 3)),
                dma((2, 2)),
                pltpu.SemaphoreType.REGULAR((2,)),
                dma((2, 4, 2)), dma((2, 4, 2)),
                dma((2, 2, 6)), dma((2, 2, 6)),
                dma((2, 2, 3)), dma((2, 2, 3)),
                dma((2, 4)), dma((2, 4)),
                dma((2, 4, 4)), dma((2, 4, 4)),
                dma((2, 4, 4)), dma((2, 4, 4)),
            ],
            compiler_params=pltpu.CompilerParams(
                collective_id=0, has_side_effects=True, vmem_limit_bytes=VMEM_LIMIT
            ),
            cost_estimate=pl.CostEstimate(flops=flops, bytes_accessed=80 * MIB, transcendentals=rows * f),
        )(x, dy, gate, up, w_gate, w_up, w_down)
        return pl.pallas_call(
            put_out,
            out_shape=tuple(jax.ShapeDtypeStruct(h.shape, h.dtype) for h in held),
            in_specs=[pl.BlockSpec(memory_space=pltpu.VMEM)] * 4,
            out_specs=[pl.BlockSpec(memory_space=pltpu.HBM)] * 4,
            scratch_shapes=[dma((4, PARTS))],
            compiler_params=pltpu.CompilerParams(vmem_limit_bytes=2 * MIB),
        )(*held)

    tokens, columns, rows = P("dp", None), P(None, "tp"), P("tp", None)
    return jax.shard_map(
        step,
        mesh=mesh,
        in_specs=(tokens, tokens, P("dp", "tp"), P("dp", "tp"), columns, columns, rows),
        out_specs=(tokens, P("dp", "tp"), P("dp", "tp"), P(("dp", "tp"), None)),
        check_vma=False,
    )


VMEM_LIMIT = 37 * MIB
```
